32 devices in a mesh: gx: 8 (over z, y), gy: 4 (over x, core).
Axes of the slice: x: 2, y: 2, z: 4, core: 2. Of those that a mesh axis runs over, the one named last changes fastest.
Arguments:
- three_index: bfloat16 [8, 4608, 4608], P('gx', 'gy'), as said below
- old_density: bfloat16 [4608, 4608], P('gy'), as said below
- core: float32 [4608, 4608], P('gy', 'gx'), as said below
Outputs:
- purified: bfloat16 [4608, 4608], P('gy', 'gx')
- idempotency: float32 [2], replicated
Inputs may be any that keep to these rules, and one draw needn't show every extreme that they name: Each slab three_index[P] is symmetric in its two basis indices. `old_density`: symmetric. `core`: symmetric.
All inputs are finite; a program needn't handle non-finite values.
Results may differ from the reference program's by a relative error of at most 0.015.
Values may be sent and summed in bfloat16 or wider, within the bound.
A program may use at most 128 MiB of HBM per device.

```python
import jax
import jax.numpy as jnp
from jax import lax

N = 4608
AUX_DEV = 1
AUX = 8
ITERS = 2
N_GX = 8


def symmetric_normal(key, shape, scale):
    values = jax.random.normal(key, shape, jnp.float32)
    values = (values + jnp.swapaxes(values, -1, -2)) * 0.5 ** 0.5
    return jnp.clip(values, -6.0, 6.0) * scale


def draw_three_index(key, part):
    scale = (N * N * AUX) ** (-0.25)
    return symmetric_normal(jax.random.fold_in(key, 11), (AUX, N, N), scale).astype(jnp.bfloat16)


def draw_old_density(key, part):
    return symmetric_normal(jax.random.fold_in(key, 12), (N, N), 1.0).astype(jnp.bfloat16)


def draw_core(key, part):
    base = symmetric_normal(jax.random.fold_in(key, 13), (N, N), 1.0)
    place = jnp.arange(N, dtype=jnp.float32) / jnp.float32(N - 1)
    squares = 0.2 + 2.6 * place
    levels = 4.0 * place * place
    amplitude = jnp.sqrt(squares)
    scaled = base * amplitude[:, None] * amplitude[None, :]
    return scaled + jnp.diag(levels * jnp.sqrt(jnp.float32(N)))


def setup_inputs(seed: int = 0) -> dict:
    keys = jax.random.split(jax.random.key(seed), 4)
    three_index = draw_three_index(jax.random.fold_in(keys[3], 71), 0)
    old_density = draw_old_density(jax.random.fold_in(keys[3], 71), 0)
    core = draw_core(jax.random.fold_in(keys[3], 71), 0)
    return {"three_index": three_index, "old_density": old_density, "core": core}


def mult(left, right):
    return jnp.dot(left.astype(jnp.float32), right.astype(jnp.float32), precision=lax.Precision.HIGHEST)

def reference(three_index, old_density, core):
    dens = old_density.astype(jnp.float32)

    def coeff(slab):
        return jnp.sum(slab.astype(jnp.float32) * dens)
    fitted = lax.map(coeff, three_index)
    fitted16 = fitted.astype(jnp.bfloat16).astype(jnp.float32)
    grouped = three_index.reshape(N_GX, AUX_DEV, N, N)
    weights = fitted16.reshape(N_GX, AUX_DEV)

    def add_group(total, pair):
        slabs, coefs = pair
        part = jnp.einsum('p,prc->rc', coefs, slabs.astype(jnp.float32), precision=lax.Precision.HIGHEST)
        part = lax.optimization_barrier(part.astype(jnp.bfloat16))
        return (total + part.astype(jnp.float32), None)
    coulomb, _ = lax.scan(add_group, jnp.zeros((N, N), jnp.float32), (grouped, weights))
    fock = core + coulomb
    eye = jnp.eye(N, dtype=jnp.float32)
    shift = jnp.trace(fock) / N
    spread = jnp.sum((fock - shift * eye) ** 2) / (N * N)
    current = ((shift * eye - fock) / (4.0 * jnp.sqrt(spread + 1e-06))).astype(jnp.bfloat16)
    scale = 1.0 / jnp.sqrt(jnp.float32(N))
    traces = []
    for step in range(ITERS):
        square_full = mult(current, current) * scale
        traces.append(jnp.trace(square_full))
        square = square_full.astype(jnp.bfloat16)
        cube = mult(square, current) * scale
        current = (1.5 * current.astype(jnp.float32) - 2.0 * cube).astype(jnp.bfloat16)
    idempotency = 16.0 * (0.25 - jnp.stack(traces) / (N * jnp.sqrt(jnp.float32(N))))
    return (current, idempotency)
```

```python
import functools

import jax
import jax.numpy as jnp
from jax import lax
from jax.experimental import pallas as pl
from jax.experimental.pallas import tpu as pltpu
from jax.sharding import PartitionSpec as P

ITERS = 2


def ring_index(position, n):
    low = (position < n // 2).astype(jnp.int32)
    return low * (2 * position) + (1 - low) * (2 * (n - 1 - position) + 1)


def gather_kernel(
    n, m, cur_t, cur, panel, right, own_t, own, load_sem, keep_sem, send_sem, recv_sem, col_send, col_recv
):
    gx = lax.axis_index("gx")
    gy = lax.axis_index("gy")
    cols = cur_t.shape[0]
    rows = cur.shape[0]
    odd = lax.rem(gx, 2)
    place = (1 - odd) * (gx // 2) + odd * (n - 1 - gx // 2)
    ahead = ring_index(lax.rem(place + 1, n), n)
    behind = ring_index(lax.rem(place + n - 1, n), n)

    barrier = pltpu.get_barrier_semaphore()
    for other in (ahead, behind):
        pl.semaphore_signal(barrier, inc=1, device_id={"gx": other})
    for k in range(1, m):
        pl.semaphore_signal(barrier, inc=1, device_id={"gy": lax.rem(gy + k, m)})
    pl.semaphore_wait(barrier, m + 1)

    def block(owner):
        return panel.at[pl.ds(pl.multiple_of(owner * cols, cols), cols), :]

    def hop(way, step):
        source = lax.rem(place + (n - step if way == 0 else step), n)
        owner = ring_index(source, n)
        return pltpu.make_async_remote_copy(
            src_ref=cur_t if step == 0 else block(owner),
            dst_ref=block(owner),
            send_sem=send_sem.at[way, step],
            recv_sem=recv_sem.at[way, step],
            device_id={"gx": ahead if way == 0 else behind},
        )

    counts = (n // 2, n - 1 - n // 2)
    hops = [[hop(way, step) for step in range(counts[way])] for way in (0, 1)]
    for way in (0, 1):
        hops[way][0].start()
    mine = right.at[pl.ds(pl.multiple_of(gy * rows, rows), rows), :]
    spread = [
        pltpu.make_async_remote_copy(
            src_ref=cur,
            dst_ref=mine,
            send_sem=col_send.at[k - 1],
            recv_sem=col_recv.at[k - 1],
            device_id={"gy": lax.rem(gy + k, m)},
        )
        for k in range(1, m)
    ]
    for copy in spread:
        copy.start()
    loads = [
        pltpu.make_async_copy(cur_t, own_t, load_sem.at[0]),
        pltpu.make_async_copy(cur, own, load_sem.at[1]),
    ]
    keeps = [
        pltpu.make_async_copy(own_t, block(gx), keep_sem.at[0]),
        pltpu.make_async_copy(own, mine, keep_sem.at[1]),
    ]
    for copy in loads:
        copy.start()
    for load, keep in zip(loads, keeps):
        load.wait()
        keep.start()
    for step in range(counts[0]):
        for way in (0, 1):
            if step < counts[way]:
                hops[way][step].wait_recv()
                if step + 1 < counts[way]:
                    hops[way][step + 1].start()
    for way in (0, 1):
        for copy in hops[way]:
            copy.wait_send()
    for copy in spread:
        copy.wait()
    for keep in keeps:
        keep.wait()


def gather(cur_t, cur, n, m, ident):
    cols, rows = cur_t.shape
    return pl.pallas_call(
        functools.partial(gather_kernel, n, m),
        out_shape=(
            jax.ShapeDtypeStruct((n * cols, rows), cur.dtype),
            jax.ShapeDtypeStruct((m * rows, cols), cur.dtype),
        ),
        in_specs=[pl.BlockSpec(memory_space=pltpu.HBM)] * 2,
        out_specs=(pl.BlockSpec(memory_space=pltpu.HBM),) * 2,
        scratch_shapes=[
            pltpu.VMEM((cols, rows), cur.dtype),
            pltpu.VMEM((rows, cols), cur.dtype),
            pltpu.SemaphoreType.DMA((2,)),
            pltpu.SemaphoreType.DMA((2,)),
            pltpu.SemaphoreType.DMA((2, n // 2)),
            pltpu.SemaphoreType.DMA((2, n // 2)),
            pltpu.SemaphoreType.DMA((m - 1,)),
            pltpu.SemaphoreType.DMA((m - 1,)),
        ],
        compiler_params=pltpu.CompilerParams(collective_id=ident, has_side_effects=True),
    )(cur_t, cur)


def scatter_kernel(n, parts, out, own, sums, landed, load_sem, send_sem, recv_sem):
    gx = lax.axis_index("gx")
    cols = out.shape[0]
    odd = lax.rem(gx, 2)
    place = (1 - odd) * (gx // 2) + odd * (n - 1 - gx // 2)
    ahead = ring_index(lax.rem(place + 1, n), n)
    behind = ring_index(lax.rem(place + n - 1, n), n)
    barrier = pltpu.get_barrier_semaphore()
    for other in (ahead, behind):
        pl.semaphore_signal(barrier, inc=1, device_id={"gx": other})
    pl.semaphore_wait(barrier, 2)

    counts = (n // 2, n - 1 - n // 2)
    starts = (0, n // 2)
    order = [(way, step) for step in range(counts[0]) for way in (0, 1) if step < counts[way]]

    def slot(way, step):
        return starts[way] + step

    def target(way, step):
        far = counts[way] - step
        return ring_index(lax.rem(place + (far if way == 0 else n - far), n), n)

    def load(owner, k):
        return pltpu.make_async_copy(
            parts.at[pl.ds(pl.multiple_of(owner * cols, cols), cols), :], own.at[k], load_sem.at[k]
        )

    def hop(way, step):
        k = slot(way, step)
        return pltpu.make_async_remote_copy(
            src_ref=own.at[k] if step == 0 else sums.at[k],
            dst_ref=landed.at[k],
            send_sem=send_sem.at[k],
            recv_sem=recv_sem.at[k],
            device_id={"gx": ahead if way == 0 else behind},
        )

    loads = {key: load(target(*key), slot(*key)) for key in order}
    loads["mine"] = load(gx, n - 1)
    for copy in loads.values():
        copy.start()
    hops = {key: hop(*key) for key in order}
    tile = next(t for t in (64, 48, 32, 16, 8) if cols % t == 0)
    for way, step in order:
        loads[way, step].wait()
        if step > 0:
            k = slot(way, step)
            hops[way, step - 1].wait_recv()

            @pl.loop(0, cols // tile)
            def _(r):
                at = pl.ds(pl.multiple_of(r * tile, tile), tile)
                total = own[k, at, :].astype(jnp.float32) + landed[k - 1, at, :].astype(jnp.float32)
                sums[k, at, :] = total.astype(sums.dtype)

        hops[way, step].start()
    loads["mine"].wait()
    ends = [slot(way, counts[way] - 1) for way in (0, 1)]
    for way in (0, 1):
        hops[way, counts[way] - 1].wait_recv()

    @pl.loop(0, cols // tile)
    def _(r):
        at = pl.ds(pl.multiple_of(r * tile, tile), tile)
        total = own[n - 1, at, :].astype(jnp.float32)
        for k in ends:
            total = total + landed[k, at, :].astype(jnp.float32)
        out[at, :] = total

    for copy in hops.values():
        copy.wait_send()


def scatter(parts, n, ident):
    cols, rows = parts.shape[0] // n, parts.shape[1]
    return pl.pallas_call(
        functools.partial(scatter_kernel, n),
        out_shape=jax.ShapeDtypeStruct((cols, rows), jnp.float32),
        in_specs=[pl.BlockSpec(memory_space=pltpu.HBM)],
        out_specs=pl.BlockSpec(memory_space=pltpu.VMEM),
        scratch_shapes=[
            pltpu.VMEM((n, cols, rows), parts.dtype),
            pltpu.VMEM((n - 1, cols, rows), parts.dtype),
            pltpu.VMEM((n - 1, cols, rows), parts.dtype),
            pltpu.SemaphoreType.DMA((n,)),
            pltpu.SemaphoreType.DMA((n - 1,)),
            pltpu.SemaphoreType.DMA((n - 1,)),
        ],
        compiler_params=pltpu.CompilerParams(
            collective_id=ident, has_side_effects=True, vmem_limit_bytes=48 * 1024 * 1024
        ),
    )(parts)


def merge_kernel(n, m, x_ref, o_ref, held, landed, send_sem, recv_sem):
    partners = []
    for axis, size in (("gy", m), ("gx", n)):
        me = lax.axis_index(axis)
        bit = 1
        while bit < size:
            partners.append({axis: me + bit * (1 - 2 * lax.rem(me // bit, 2))})
            bit *= 2
    barrier = pltpu.get_barrier_semaphore()
    for other in partners:
        pl.semaphore_signal(barrier, inc=1, device_id=other)
    pl.semaphore_wait(barrier, len(partners))
    held[0] = x_ref[...]
    for k, other in enumerate(partners):
        copy = pltpu.make_async_remote_copy(
            src_ref=held.at[k],
            dst_ref=landed.at[k],
            send_sem=send_sem.at[k],
            recv_sem=recv_sem.at[k],
            device_id=other,
        )
        copy.start()
        copy.wait()
        a, b = held[k], landed[k]
        gap = a[1] / jnp.maximum(a[2], 1.0) - b[1] / jnp.maximum(b[2], 1.0)
        weight = a[2] * b[2] / jnp.maximum(a[2] + b[2], 1.0)
        held[k + 1, 0] = a[0] + b[0] + weight * (gap * gap)
        held[k + 1, 1] = a[1] + b[1]
        held[k + 1, 2] = a[2] + b[2]
    o_ref[...] = held[len(partners)]


def merge(squares, total, count, n, m, ident):
    x = jnp.broadcast_to(
        jnp.stack([squares, total, count]).astype(jnp.float32)[:, None, None], (3, 8, 128)
    )
    steps = (n - 1).bit_length() + (m - 1).bit_length()
    out = pl.pallas_call(
        functools.partial(merge_kernel, n, m),
        out_shape=jax.ShapeDtypeStruct(x.shape, x.dtype),
        in_specs=[pl.BlockSpec(memory_space=pltpu.VMEM)],
        out_specs=pl.BlockSpec(memory_space=pltpu.VMEM),
        scratch_shapes=[
            pltpu.VMEM((steps + 1, 3, 8, 128), jnp.float32),
            pltpu.VMEM((steps, 3, 8, 128), jnp.float32),
            pltpu.SemaphoreType.DMA((steps,)),
            pltpu.SemaphoreType.DMA((steps,)),
        ],
        compiler_params=pltpu.CompilerParams(collective_id=ident, has_side_effects=True),
    )(x)
    return out[0, 0, 0], out[1, 0, 0]


def per_device(n, m, three_index, old_density, core):
    aux_dev, rows, width = three_index.shape
    cols = core.shape[1]
    dens = old_density.astype(jnp.float32)
    partial_value = jnp.sum(three_index.astype(jnp.float32) * dens[None], axis=(1, 2))
    fitted = lax.psum(partial_value, "gy")
    fitted16 = fitted.astype(jnp.bfloat16)
    parts = jnp.einsum(
        "p,prc->cr", fitted16, three_index, preferred_element_type=jnp.float32
    ).astype(jnp.bfloat16)
    coulomb = scatter(parts, n, 2 + ITERS)
    fock = core + coulomb.T
    row_start = lax.axis_index("gy") * rows
    col_start = lax.axis_index("gx") * cols
    row_ids = row_start + lax.broadcasted_iota(jnp.int32, (rows, cols), 0)
    col_ids = col_start + lax.broadcasted_iota(jnp.int32, (rows, cols), 1)
    diagonal = row_ids == col_ids
    diag_mask = diagonal.astype(jnp.float32)
    count = jnp.maximum(
        jnp.minimum(row_start + rows, col_start + cols) - jnp.maximum(row_start, col_start), 0
    ).astype(jnp.float32)
    local_trace = jnp.sum(jnp.where(diagonal, fock, 0.0))
    centred = fock - (local_trace / jnp.maximum(count, 1.0)) * diag_mask
    squares, trace = merge(jnp.sum(centred * centred), local_trace, count, n, m, 0)
    shift = trace / width
    spread = squares / (width * width)
    current = ((shift * diag_mask - fock) / (4.0 * jnp.sqrt(spread + 1e-06))).astype(jnp.bfloat16)
    scale = 1.0 / jnp.sqrt(jnp.float32(width))
    contract = (((0,), (0,)), ((), ()))
    traces = []
    for step in range(ITERS):
        panel, right = gather(current.T, current, n, m, 1 + step)
        square_full = lax.dot_general(panel, right, contract, preferred_element_type=jnp.float32) * scale
        square = square_full.astype(jnp.bfloat16)
        square_block = lax.all_gather(square, "gy", axis=0, tiled=True)
        cube = lax.dot_general(panel, square_block, contract, preferred_element_type=jnp.float32) * scale
        traces.append(jnp.sum(jnp.where(diagonal, square_full, 0.0)))
        current = (1.5 * current.astype(jnp.float32) - 2.0 * cube).astype(jnp.bfloat16)
    last, first = merge(traces[1], traces[0], jnp.float32(0), n, m, 1 + ITERS)
    idempotency = 16.0 * (0.25 - jnp.stack([first, last]) / (width * jnp.sqrt(jnp.float32(width))))
    return (current, idempotency)


def solution(mesh):
    placed = (P("gx", "gy", None), P("gy", None), P("gy", "gx"))
    return jax.shard_map(
        functools.partial(per_device, mesh.shape["gx"], mesh.shape["gy"]),
        mesh=mesh,
        in_specs=placed,
        out_specs=(P("gy", "gx"), P()),
        check_vma=False,
    )
```
